32 devices in a mesh: frames: 8 (over y, x, core), atoms: 4 (over z).
Axes of the slice: x: 2, y: 2, z: 4, core: 2. Of those that a mesh axis runs over, the one named last changes fastest.
Arguments:
- frames: float32 [512, 3, 6144], P('frames', None, 'atoms'), may hold values from -45 to 45, as said below
- reference_structure: float32 [3, 6144], P(None, 'atoms'), may hold values from -15 to 15
Outputs:
- covariance: float32 [3, 6144, 3, 6144], P(None, 'frames', None, 'atoms')
- mean_structure: float32 [3, 6144], P(None, 'atoms')
The draws below stay inside these ranges and needn't reach their ends.
Inputs may be any that keep to these rules, and one draw needn't show every extreme that they name: `frames`: every frame, once centered, has a cross-covariance with the centered reference_structure of positive determinant whose singular values lie within a factor of 20 of one another.
All inputs are finite; a program needn't handle non-finite values.
Results may differ from the reference program's by a relative error of at most 0.0003.
Values may be sent and summed in bfloat16 or wider, within the bound.
No kernel may reach another device: no remote copies, remote signals or barrier semaphores. Data moves between devices by JAX's collectives and lax.ppermute only.
A program may use at most 192 MiB of HBM per device.

```python
import jax
import jax.numpy as jnp
from jax import lax

ATOMS = 6144
ITERS = 2
POLAR = 8
FRAMES = 512


def base_structure(key):
    points = jax.random.normal(jax.random.fold_in(key, 101), (3, ATOMS), jnp.float32)
    spread = jnp.array([3.0, 3.0, 3.0], jnp.float32)
    return jnp.clip(points * spread[:, None], -12.0, 12.0)


def unit_vector(key, salt):
    raw = jax.random.normal(jax.random.fold_in(key, salt), (3,), jnp.float32)
    return raw / jnp.sqrt(jnp.sum(raw * raw) + 1e-12)


def hinge_setup(key):
    base = base_structure(key)
    first_axis = unit_vector(key, 111)
    other_axis = unit_vector(key, 112)
    other_axis = other_axis - jnp.sum(other_axis * first_axis) * first_axis
    other_axis = other_axis / jnp.sqrt(jnp.sum(other_axis * other_axis) + 1e-12)
    facing = unit_vector(key, 113)
    domain = (jnp.sum(facing[:, None] * base, axis=0) > 0.0).astype(jnp.float32)
    return (base, first_axis, other_axis, domain)


def axis_rotation(axis, angle):
    zero = jnp.zeros((), jnp.float32)
    generator = jnp.stack([jnp.stack([zero, -axis[2], axis[1]]), jnp.stack([axis[2], zero, -axis[0]]), jnp.stack([-axis[1], axis[0], zero])])
    generator_sq = jnp.dot(generator, generator, precision=jax.lax.Precision.HIGHEST)
    return jnp.eye(3, dtype=jnp.float32)[None] + jnp.sin(angle)[:, None, None] * generator[None] + (1.0 - jnp.cos(angle))[:, None, None] * generator_sq[None]


def hinged(base, domain, turns):
    rotated = jnp.einsum('nij,ja->nia', turns, base, precision=jax.lax.Precision.HIGHEST)
    return base[None] + domain[None, None, :] * (rotated - base[None])


def draw_reference_structure(key, part):
    base, first_axis, other_axis, domain = hinge_setup(key)
    magnitude = jax.random.uniform(jax.random.fold_in(key, 203), (1,), jnp.float32, 0.6, 0.9)
    flip_sign = jnp.where(jax.random.uniform(jax.random.fold_in(key, 204), (1,), jnp.float32) < 0.5, -1.0, 1.0)
    shaped = hinged(base, domain, axis_rotation(other_axis, magnitude * flip_sign))[0]
    jitter = jnp.clip(0.5 * jax.random.normal(jax.random.fold_in(key, 202), (3, ATOMS), jnp.float32), -3.0, 3.0)
    return jnp.clip(shaped + jitter, -15.0, 15.0)


def draw_frames(key, part):
    base, first_axis, other_axis, domain = hinge_setup(key)
    swings = jnp.clip(0.7 * jax.random.normal(jax.random.fold_in(key, 309), (FRAMES,), jnp.float32), -1.2, 1.2)
    shaped = hinged(base, domain, axis_rotation(first_axis, swings))
    atom_spread = jnp.exp(jax.random.uniform(jax.random.fold_in(key, 303), (ATOMS,), jnp.float32, jnp.log(0.3), jnp.log(1.5)))
    noise = jax.random.normal(jax.random.fold_in(key, 304), (FRAMES, 3, ATOMS), jnp.float32) * atom_spread[None, None, :]
    noise = jnp.clip(noise, -6.0, 6.0)
    quats = jax.random.normal(jax.random.fold_in(key, 307), (FRAMES, 4), jnp.float32)
    quats = quats / jnp.sqrt(jnp.sum(quats * quats, axis=1, keepdims=True) + 1e-12)
    a, b, c, d = (quats[:, 0], quats[:, 1], quats[:, 2], quats[:, 3])
    rotation = jnp.stack([jnp.stack([1 - 2 * (c * c + d * d), 2 * (b * c - d * a), 2 * (b * d + c * a)], axis=1), jnp.stack([2 * (b * c + d * a), 1 - 2 * (b * b + d * d), 2 * (c * d - b * a)], axis=1), jnp.stack([2 * (b * d - c * a), 2 * (c * d + b * a), 1 - 2 * (b * b + c * c)], axis=1)], axis=1)
    moved = jnp.einsum('fij,fja->fia', rotation, shaped + noise, precision=jax.lax.Precision.HIGHEST)
    offset = jnp.clip(5.0 * jax.random.normal(jax.random.fold_in(key, 308), (FRAMES, 3, 1), jnp.float32), -10.0, 10.0)
    return jnp.clip(moved + offset, -45.0, 45.0)


def setup_inputs(seed: int = 0) -> dict:
    seeds = jax.random.split(jax.random.key(seed), 3)
    return {
        "frames": draw_frames(jax.random.fold_in(seeds[2], 71), 0),
        "reference_structure": draw_reference_structure(jax.random.fold_in(seeds[2], 71), 0),
    }


def polar_factor(cross):
    factor = jnp.sqrt(3.0 / lax.optimization_barrier(jnp.sum(cross * cross, axis=(0, 1))))
    matrix = cross * factor[None, None, :]
    for turn in range(POLAR):
        entries = [[matrix[i, j] for j in range(3)] for i in range(3)]
        cofactor = [[entries[(i + 1) % 3][(j + 1) % 3] * entries[(i + 2) % 3][(j + 2) % 3] - entries[(i + 1) % 3][(j + 2) % 3] * entries[(i + 2) % 3][(j + 1) % 3] for j in range(3)] for i in range(3)]
        determinant = entries[0][0] * cofactor[0][0] + entries[0][1] * cofactor[0][1] + entries[0][2] * cofactor[0][2]
        inverse = jnp.stack([jnp.stack(cofactor[i]) for i in range(3)]) / determinant[None, None, :]
        matrix = 0.5 * (matrix + inverse)
    return matrix

def reference(frames, reference_structure):
    highest = lax.Precision.HIGHEST
    mean_now = reference_structure
    for iteration in range(ITERS):
        centroid = lax.optimization_barrier(jnp.sum(frames, axis=2)) / ATOMS
        shifted = frames - centroid[:, :, None]
        cross = jnp.einsum('fca,da->cdf', shifted, mean_now, precision=highest)
        rotation = polar_factor(cross)
        aligned = jnp.einsum('cdf,fca->fda', rotation, shifted, precision=highest)
        mean_now = lax.optimization_barrier(jnp.sum(aligned, axis=0)) / FRAMES
    deviation = (aligned - mean_now[None]).astype(jnp.bfloat16).reshape(FRAMES, 3 * ATOMS)
    product = lax.dot_general(deviation, deviation, (((0,), (0,)), ((), ())), preferred_element_type=jnp.float32)
    covariance = (product / FRAMES).reshape(3, ATOMS, 3, ATOMS)
    return (covariance, mean_now)
```

```python
import functools

import jax
import jax.numpy as jnp
from jax import lax
from jax.experimental import pallas as pl
from jax.experimental.pallas import tpu as pltpu
from jax.sharding import PartitionSpec as P

ITERS = 2
POLAR = 8
TILE = 128


def polar_factor(cross):
    factor = jnp.sqrt(3.0 / jnp.sum(cross * cross, axis=(0, 1)))
    matrix = cross * factor[None, None, :]
    for turn in range(POLAR):
        entries = [[matrix[i, j] for j in range(3)] for i in range(3)]
        cofactor = [
            [
                entries[(i + 1) % 3][(j + 1) % 3] * entries[(i + 2) % 3][(j + 2) % 3]
                - entries[(i + 1) % 3][(j + 2) % 3] * entries[(i + 2) % 3][(j + 1) % 3]
                for j in range(3)
            ]
            for i in range(3)
        ]
        determinant = (
            entries[0][0] * cofactor[0][0]
            + entries[0][1] * cofactor[0][1]
            + entries[0][2] * cofactor[0][2]
        )
        inverse = jnp.stack([jnp.stack(cofactor[i]) for i in range(3)]) / determinant[None, None, :]
        matrix = 0.5 * (matrix + inverse)
    return matrix


def superpose(coords, reference_structure, atoms, count_all):
    highest = lax.Precision.HIGHEST
    mean_now = reference_structure
    for iteration in range(ITERS):
        sum_coords, sum_cross, sum_mean = lax.psum(
            (
                jnp.sum(coords, axis=2),
                jnp.einsum("cfa,da->cdf", coords, mean_now, precision=highest),
                jnp.sum(mean_now, axis=1),
            ),
            "atoms",
        )
        centroid = sum_coords / atoms
        cross = sum_cross - centroid[:, None, :] * sum_mean[None, :, None]
        shifted = coords - centroid[:, :, None]
        rotation = polar_factor(cross)
        aligned = jnp.einsum("cdf,cfa->dfa", rotation, shifted, precision=highest)
        partial = lax.all_gather(jnp.sum(aligned, axis=1), "frames", axis=0)
        mean_now = jnp.sum(partial, axis=0) / count_all
    return (aligned - mean_now[:, None]).astype(jnp.bfloat16), mean_now


def product_kernel(count, scale_exact, info, *refs):
    blocks = refs[: 4 * count]
    out, columns, rows = refs[4 * count :]
    same, partner = blocks[:count], blocks[count : 2 * count]
    row_same, row_partner = blocks[2 * count : 3 * count], blocks[3 * count :]
    frames_here = same[0].shape[1]
    row_count = rows.shape[2]
    core, plane, is_hub = info[0], info[1], info[2]
    start = pl.multiple_of(core * row_count, row_count)

    @pl.when((pl.program_id(0) == 0) & (pl.program_id(1) == 0))
    def _():
        for s in range(count):
            for e, blk in ((0, same[s]), (1, partner[s])):
                slot = (2 * s + e) * frames_here
                columns[:, slot : slot + frames_here, :] = blk[...]

        @pl.when(is_hub == 1)
        def _():
            rows[...] = columns[:, :, pl.ds(start, row_count)]

        @pl.when(is_hub == 0)
        def _():
            for t in range(count):
                for e, blk in ((0, row_same[t]), (1, row_partner[t])):
                    slot = pl.multiple_of((2 * (plane ^ t) + e) * frames_here, frames_here)
                    rows[:, pl.ds(slot, frames_here), :] = blk[:, :, pl.ds(start, row_count)]

    first = pl.multiple_of(pl.program_id(1) * TILE, TILE)
    left = rows[pl.program_id(0), :, pl.ds(first, TILE)]
    total = columns.shape[1]
    for d in range(3):
        value = lax.dot_general(
            left, columns[d], (((0,), (0,)), ((), ())), preferred_element_type=jnp.float32
        )
        out[0, d] = value * (1.0 / scale_exact) if scale_exact & (scale_exact - 1) == 0 else value / scale_exact


def covariance_of(info, blocks, row_count, count_all):
    count = len(blocks) // 4
    frames_here, column_atoms = blocks[0].shape[1], blocks[0].shape[2]
    total = 2 * count * frames_here
    return pl.pallas_call(
        functools.partial(product_kernel, count, count_all),
        out_shape=jax.ShapeDtypeStruct((3, 3, row_count, column_atoms), jnp.float32),
        grid=(3, row_count // TILE),
        in_specs=[pl.BlockSpec(memory_space=pltpu.SMEM)]
        + [pl.BlockSpec(memory_space=pltpu.VMEM)] * len(blocks),
        out_specs=pl.BlockSpec((1, 3, TILE, column_atoms), lambda c, i: (c, 0, i, 0)),
        scratch_shapes=[
            pltpu.VMEM((3, total, column_atoms), jnp.bfloat16),
            pltpu.VMEM((3, total, row_count), jnp.bfloat16),
        ],
        compiler_params=pltpu.CompilerParams(
            dimension_semantics=("arbitrary", "arbitrary"), vmem_limit_bytes=56 * 2**20
        ),
        cost_estimate=pl.CostEstimate(
            flops=2 * total * 9 * row_count * column_atoms,
            bytes_accessed=36 * row_count * column_atoms,
            transcendentals=0,
        ),
    )(info, *blocks)


def direct(deviation, planes, row_count, count_all):
    def device(q, c, z):
        return (2 * q + c) * planes + z

    both = ("frames", "atoms")
    every = range(planes)
    swap = [(i, i ^ 1) for i in range(2 * planes)]
    row_same = [
        lax.ppermute(
            deviation,
            both,
            [
                (device(q ^ t ^ z, c, q), device(q, c, z))
                for q in every
                for c in range(2)
                for z in every
                if z != q
            ],
        )
        for t in every
    ]
    same = [deviation] + [
        lax.ppermute(deviation, "frames", [(2 * (q ^ s) + c, 2 * q + c) for q in every for c in range(2)])
        for s in every
        if s
    ]
    partner = [lax.ppermute(block, "frames", swap) for block in same]
    row_partner = [lax.ppermute(block, "frames", swap) for block in row_same]
    place, plane = lax.axis_index("frames"), lax.axis_index("atoms")
    info = jnp.stack([place % 2, plane, (place // 2 == plane).astype(jnp.int32)]).astype(jnp.int32)
    product = covariance_of(info, [*same, *partner, *row_same, *row_partner], row_count, count_all)
    return jnp.transpose(product, (0, 2, 1, 3))


def general(deviation, row_count, count_all):
    panel = lax.all_gather(deviation, "frames", axis=1, tiled=True)
    ratio = lax.axis_size("frames") // lax.axis_size("atoms")
    place = lax.axis_index("frames")
    selected = lax.dynamic_slice_in_dim(panel, place % ratio * row_count, row_count, 2)
    mine = lax.axis_index("atoms") == place // ratio
    rows = lax.psum(jnp.where(mine, selected, jnp.zeros_like(selected)), "atoms")
    product = jnp.einsum("cfa,dfb->cadb", rows, panel, preferred_element_type=jnp.float32)
    return product / count_all


def body(frames, reference_structure):
    coords = jnp.transpose(frames, (1, 0, 2))
    planes, places = lax.axis_size("atoms"), lax.axis_size("frames")
    column_atoms = frames.shape[2]
    atoms = column_atoms * planes
    count_all = frames.shape[0] * places
    row_count = atoms // places
    deviation, mean = superpose(coords, reference_structure, atoms, count_all)
    if places == 2 * planes and planes <= 4 and planes & (planes - 1) == 0 and row_count % TILE == 0:
        covariance = direct(deviation, planes, row_count, count_all)
    else:
        covariance = general(deviation, row_count, count_all)
    return covariance, mean


def solution(mesh):
    return jax.shard_map(
        body,
        mesh=mesh,
        in_specs=(P("frames", None, "atoms"), P(None, "atoms")),
        out_specs=(P(None, "frames", None, "atoms"), P(None, "atoms")),
        check_vma=False,
    )
```

```python
import functools

import jax
import jax.numpy as jnp
from jax import lax
from jax.experimental import pallas as pl
from jax.experimental.pallas import tpu as pltpu
from jax.sharding import PartitionSpec as P


ITERS = 2
POLAR = 8
TILE = 256
SLOTS = 4


def polar_factor(cross):
    factor = jnp.sqrt(3.0 / jnp.sum(cross * cross, axis=(0, 1)))
    matrix = cross * factor[None, None, :]
    for _ in range(POLAR):
        entries = [[matrix[i, j] for j in range(3)] for i in range(3)]
        cofactor = [
            [
                entries[(i + 1) % 3][(j + 1) % 3] * entries[(i + 2) % 3][(j + 2) % 3]
                - entries[(i + 1) % 3][(j + 2) % 3] * entries[(i + 2) % 3][(j + 1) % 3]
                for j in range(3)
            ]
            for i in range(3)
        ]
        determinant = (
            entries[0][0] * cofactor[0][0]
            + entries[0][1] * cofactor[0][1]
            + entries[0][2] * cofactor[0][2]
        )
        inverse = jnp.stack([jnp.stack(cofactor[i]) for i in range(3)]) / determinant[None, None, :]
        matrix = 0.5 * (matrix + inverse)
    return matrix


def sum_over(value, axis, steps):
    size = lax.axis_size(axis)
    if size & (size - 1) or size > 16:
        return lax.psum(value, axis)
    for masks in steps:
        value = value + sum(lax.ppermute(value, axis, [(i, i ^ m) for i in range(size)]) for m in masks)
    return value


def powers(size):
    return [[1], range(2, size, 2)] if size > 2 else [range(1, size)]


def superpose(coords, reference_structure, atoms, count_all):
    highest = lax.Precision.HIGHEST
    count = coords.shape[1]
    mean_now = reference_structure
    for iteration in range(ITERS):
        parts = [
            jnp.einsum("cfa,da->cdf", coords, mean_now, precision=highest).reshape(9, count),
            jnp.broadcast_to(jnp.sum(mean_now, axis=1)[:, None], (3, count)),
        ]
        if iteration == 0:
            parts.append(jnp.sum(coords, axis=2))
        totals = sum_over(jnp.concatenate(parts), "atoms", [range(1, lax.axis_size("atoms"))])
        if iteration == 0:
            centroid = totals[12:15] / atoms
            shifted = coords - centroid[:, :, None]
        cross = totals[:9].reshape(3, 3, count) - centroid[:, None, :] * totals[9:12][None]
        rotation = polar_factor(cross)
        aligned = jnp.einsum("cdf,cfa->dfa", rotation, shifted, precision=highest)
        mean_now = sum_over(jnp.sum(aligned, axis=1), "frames", powers(lax.axis_size("frames"))) / count_all
    return (aligned - mean_now[:, None]).astype(jnp.bfloat16), mean_now


def product_kernel(count, scale, components, first, info, *refs):
    same, partner, row_blocks = refs[:count], refs[count : 2 * count], refs[2 * count : 3 * count]
    out, turned, ready, sent = refs[-4:]
    component, tile = pl.program_id(0), pl.program_id(1)
    step = 6 * component + tile
    slot = lax.rem(step, SLOTS)
    core, plane, is_hub = info[0], info[1], info[2]
    depth, row_count = same[0].shape[1], same[0].shape[2]

    def copy(c, d, half, k):
        start = pl.multiple_of(half * row_count, row_count)
        return pltpu.make_async_copy(
            ready.at[k], out.at[c + first, d, :, pl.ds(start, row_count)], sent.at[k]
        )

    @pl.when((tile == 0) & (is_hub == 1))
    def _():
        for s in range(count):
            turned[:, s * depth : (s + 1) * depth] = same[s][component + first].T

    @pl.when((tile == 0) & (is_hub == 0))
    def _():
        for t in range(count):
            start = pl.multiple_of((plane ^ t) * depth, depth)
            turned[:, pl.ds(start, depth)] = row_blocks[t][component].T

    @pl.when(step >= SLOTS)
    def _():
        copy(0, 0, 0, slot).wait()

    def multiply(blocks):
        right = jnp.concatenate([block[tile // 2] for block in blocks], axis=0)
        for m in range(0, row_count, TILE):
            value = jnp.dot(turned[m : m + TILE, :], right, preferred_element_type=jnp.float32)
            ready[slot, m : m + TILE, :] = value * (1.0 / scale) if scale & (scale - 1) == 0 else value / scale

    @pl.when(tile % 2 == 0)
    def _():
        multiply(same)

    @pl.when(tile % 2 == 1)
    def _():
        multiply(partner)

    copy(component, tile // 2, core ^ (tile % 2), slot).start()

    @pl.when(step == 6 * components - 1)
    def _():
        for k in range(SLOTS):
            copy(0, 0, 0, k).wait()


def covariance_part(info, first, components, same, partner, rows, count_all, so_far):
    count = len(same)
    depth, row_count = same[0].shape[1], same[0].shape[2]
    operands = [info, *same, *partner, *rows]
    specs = [pl.BlockSpec(memory_space=pltpu.SMEM)]
    specs += [pl.BlockSpec(memory_space=pltpu.VMEM)] * (3 * count)
    aliases = {}
    if so_far is not None:
        aliases = {len(operands): 0}
        operands.append(so_far)
        specs.append(pl.BlockSpec(memory_space=pl.ANY))
    return pl.pallas_call(
        functools.partial(product_kernel, count, count_all, components, first),
        out_shape=jax.ShapeDtypeStruct((3, 3, row_count, 2 * row_count), jnp.float32),
        grid=(components, 6),
        in_specs=specs,
        out_specs=pl.BlockSpec(memory_space=pl.ANY),
        scratch_shapes=[
            pltpu.VMEM((row_count, count * depth), jnp.bfloat16),
            pltpu.VMEM((SLOTS, row_count, row_count), jnp.float32),
            pltpu.SemaphoreType.DMA((SLOTS,)),
        ],
        input_output_aliases=aliases,
        compiler_params=pltpu.CompilerParams(
            dimension_semantics=("arbitrary", "arbitrary"), vmem_limit_bytes=48 * 2**20
        ),
        cost_estimate=pl.CostEstimate(
            flops=2 * count * depth * components * 6 * row_count * row_count,
            bytes_accessed=24 * components * row_count * row_count,
            transcendentals=0,
        ),
    )(*operands)


def direct(deviation, planes, row_count, count_all):
    def device(q, c, z):
        return (2 * q + c) * planes + z

    both = ("frames", "atoms")
    every = range(planes)
    swap = [(i, i ^ 1) for i in range(2 * planes)]
    place, plane = lax.axis_index("frames"), lax.axis_index("atoms")
    core = place % 2
    other = lax.ppermute(deviation, "frames", swap)
    lower = core == 0
    chip = jnp.concatenate([jnp.where(lower, deviation, other), jnp.where(lower, other, deviation)], axis=1)
    left, right = chip[:, :, :row_count], chip[:, :, row_count:]
    mine, theirs = jnp.where(lower, left, right), jnp.where(lower, right, left)
    mine, theirs, mine_early, mine_late = lax.optimization_barrier((mine, theirs, mine[:2], mine[2:]))

    def rows_of(block):
        return [
            lax.ppermute(
                block,
                both,
                [
                    (device(q ^ t ^ z, c, q), device(q, c, z))
                    for q in every
                    for c in range(2)
                    for z in every
                    if z != q
                ],
            )
            for t in every
        ]

    early = rows_of(mine_early)
    same = [mine] + [
        lax.ppermute(mine, "frames", [(2 * (q ^ s) + c, 2 * q + c) for q in every for c in range(2)])
        for s in every
        if s
    ]
    late = rows_of(mine_late)
    partner = [theirs] + [lax.ppermute(same[s], "frames", swap) for s in every if s]
    info = jnp.stack([core, plane, (place // 2 == plane).astype(jnp.int32)]).astype(jnp.int32)
    product = covariance_part(info, 0, 2, same, partner, early, count_all, None)
    product = covariance_part(info, 2, 1, same, partner, late, count_all, product)
    return jnp.transpose(product, (0, 2, 1, 3))


def permutes_fit(planes, places):
    return places == 2 * planes and planes <= 4 and planes & (planes - 1) == 0


def general(deviation, row_count, count_all):
    panel = lax.all_gather(deviation, "frames", axis=1, tiled=True)
    ratio = lax.axis_size("frames") // lax.axis_size("atoms")
    place = lax.axis_index("frames")
    selected = lax.dynamic_slice_in_dim(panel, place % ratio * row_count, row_count, 2)
    mine = lax.axis_index("atoms") == place // ratio
    rows = lax.psum(jnp.where(mine, selected, jnp.zeros_like(selected)), "atoms")
    product = jnp.einsum("cfa,dfb->cadb", rows, panel, preferred_element_type=jnp.float32)
    return product / count_all


def whole(frames, reference_structure):
    coords = jnp.transpose(frames, (1, 0, 2))
    planes, places = lax.axis_size("atoms"), lax.axis_size("frames")
    column_atoms = frames.shape[2]
    atoms = column_atoms * planes
    count_all = frames.shape[0] * places
    row_count = atoms // places
    deviation, mean = superpose(coords, reference_structure, atoms, count_all)
    if permutes_fit(planes, places) and row_count % TILE == 0:
        covariance = direct(deviation, planes, row_count, count_all)
    else:
        covariance = general(deviation, row_count, count_all)
    return covariance, mean


def solution(mesh):
    return jax.shard_map(
        whole,
        mesh=mesh,
        in_specs=(P("frames", None, "atoms"), P(None, "atoms")),
        out_specs=(P(None, "frames", None, "atoms"), P(None, "atoms")),
        check_vma=False,
    )
```

```python
import functools

import jax
import jax.numpy as jnp
from jax import lax
from jax.experimental import pallas as pl
from jax.experimental.pallas import tpu as pltpu
from jax.sharding import PartitionSpec as P


ITERS = 2
POLAR = 8
TILE = 256
SLOTS = 4
EARLY = 1


def polar_factor(cross):
    factor = jnp.sqrt(3.0 / jnp.sum(cross * cross, axis=(0, 1)))
    matrix = cross * factor[None, None, :]
    for _ in range(POLAR):
        entries = [[matrix[i, j] for j in range(3)] for i in range(3)]
        cofactor = [
            [
                entries[(i + 1) % 3][(j + 1) % 3] * entries[(i + 2) % 3][(j + 2) % 3]
                - entries[(i + 1) % 3][(j + 2) % 3] * entries[(i + 2) % 3][(j + 1) % 3]
                for j in range(3)
            ]
            for i in range(3)
        ]
        determinant = (
            entries[0][0] * cofactor[0][0]
            + entries[0][1] * cofactor[0][1]
            + entries[0][2] * cofactor[0][2]
        )
        inverse = jnp.stack([jnp.stack(cofactor[i]) for i in range(3)]) / determinant[None, None, :]
        matrix = 0.5 * (matrix + inverse)
    return matrix


def sum_over(value, axis, steps):
    size = lax.axis_size(axis)
    if size & (size - 1) or size > 16:
        return lax.psum(value, axis)
    for masks in steps:
        value = value + sum(lax.ppermute(value, axis, [(i, i ^ m) for i in range(size)]) for m in masks)
    return value


def powers(size):
    return [[1], range(2, size, 2)] if size > 2 else [range(1, size)]


def superpose(coords, reference_structure, atoms, count_all):
    highest = lax.Precision.HIGHEST
    count = coords.shape[1]
    mean_now = reference_structure
    for iteration in range(ITERS):
        weights = mean_now
        if iteration == 0:
            weights = jnp.concatenate([mean_now, jnp.ones_like(mean_now[:1])])
        sums = jnp.einsum("cfa,da->dcf", coords, weights, precision=highest).reshape(-1, count)
        parts = [sums, jnp.broadcast_to(jnp.sum(mean_now, axis=1)[:, None], (3, count))]
        totals = sum_over(jnp.concatenate(parts), "atoms", [range(1, lax.axis_size("atoms"))])
        if iteration == 0:
            centroid = totals[9:12] / atoms
            shifted = coords - centroid[:, :, None]
        cross = totals[:9].reshape(3, 3, count).transpose(1, 0, 2) - centroid[:, None, :] * totals[-3:][None]
        rotation = polar_factor(cross)
        if iteration == ITERS - 1:
            aligned = jnp.stack(
                [sum(rotation[c, d][:, None] * shifted[c] for c in range(3)) for d in range(3)]
            )
        else:
            aligned = jnp.einsum("cdf,cfa->dfa", rotation, shifted, precision=highest)
        mean_now = sum_over(jnp.sum(aligned, axis=1), "frames", powers(lax.axis_size("frames"))) / count_all
    return (aligned - mean_now[:, None]).astype(jnp.bfloat16), mean_now


def product_kernel(count, scale, components, first, info, *refs):
    same, partner, row_blocks = refs[:count], refs[count : 2 * count], refs[2 * count : 3 * count]
    out, turned, ready, sent = refs[-4:]
    component, tile = pl.program_id(0), pl.program_id(1)
    step = 6 * component + tile
    slot = lax.rem(step, SLOTS)
    core, plane, is_hub = info[0], info[1], info[2]
    depth, row_count = same[0].shape[1], same[0].shape[2]

    def copy(c, d, half, k, m, n):
        start = pl.multiple_of(half * row_count, row_count)
        return pltpu.make_async_copy(
            ready.at[k, m : m + n],
            out.at[c + first, d, m : m + n, pl.ds(start, row_count)],
            sent.at[k],
        )

    @pl.when((tile == 0) & (is_hub == 1))
    def _():
        for s in range(count):
            turned[:, s * depth : (s + 1) * depth] = same[s][component + first].T

    @pl.when((tile == 0) & (is_hub == 0))
    def _():
        for t in range(count):
            start = pl.multiple_of((plane ^ t) * depth, depth)
            turned[:, pl.ds(start, depth)] = row_blocks[t][component].T

    @pl.when(step >= SLOTS)
    def _():
        copy(0, 0, 0, slot, 0, row_count).wait()

    def multiply(blocks):
        right = jnp.concatenate([block[lax.rem(tile, 3)] for block in blocks], axis=0)
        for m in range(0, row_count, TILE):
            value = jnp.dot(turned[m : m + TILE, :], right, preferred_element_type=jnp.float32)
            ready[slot, m : m + TILE, :] = value * (1.0 / scale) if scale & (scale - 1) == 0 else value / scale
            copy(component, lax.rem(tile, 3), core ^ (tile // 3), slot, m, TILE).start()

    @pl.when(tile < 3)
    def _():
        multiply(same)

    @pl.when(tile >= 3)
    def _():
        multiply(partner)

    @pl.when(step == 6 * components - 1)
    def _():
        for k in range(SLOTS):
            copy(0, 0, 0, k, 0, row_count).wait()


def covariance_part(info, first, components, same, partner, rows, count_all, so_far):
    count = len(same)
    depth, row_count = same[0].shape[1], same[0].shape[2]
    operands = [info, *same, *partner, *rows]
    specs = [pl.BlockSpec(memory_space=pltpu.SMEM)]
    specs += [pl.BlockSpec(memory_space=pltpu.VMEM)] * (3 * count)
    aliases = {}
    if so_far is not None:
        aliases = {len(operands): 0}
        operands.append(so_far)
        specs.append(pl.BlockSpec(memory_space=pl.ANY))
    return pl.pallas_call(
        functools.partial(product_kernel, count, count_all, components, first),
        out_shape=jax.ShapeDtypeStruct((3, 3, row_count, 2 * row_count), jnp.float32),
        grid=(components, 6),
        in_specs=specs,
        out_specs=pl.BlockSpec(memory_space=pl.ANY),
        scratch_shapes=[
            pltpu.VMEM((row_count, count * depth), jnp.bfloat16),
            pltpu.VMEM((SLOTS, row_count, row_count), jnp.float32),
            pltpu.SemaphoreType.DMA((SLOTS,)),
        ],
        input_output_aliases=aliases,
        compiler_params=pltpu.CompilerParams(
            dimension_semantics=("arbitrary", "arbitrary"), vmem_limit_bytes=24 * 2**20
        ),
        cost_estimate=pl.CostEstimate(
            flops=2 * count * depth * components * 6 * row_count * row_count,
            bytes_accessed=24 * components * row_count * row_count,
            transcendentals=0,
        ),
    )(*operands)


def direct(deviation, planes, row_count, count_all):
    def device(q, c, z):
        return (2 * q + c) * planes + z

    both = ("frames", "atoms")
    every = range(planes)
    swap = [(i, i ^ 1) for i in range(2 * planes)]
    place, plane = lax.axis_index("frames"), lax.axis_index("atoms")
    core = place % 2
    other = lax.ppermute(deviation, "frames", swap)
    lower = core == 0
    chip = jnp.concatenate([jnp.where(lower, deviation, other), jnp.where(lower, other, deviation)], axis=1)
    left, right = chip[:, :, :row_count], chip[:, :, row_count:]
    mine, theirs = jnp.where(lower, left, right), jnp.where(lower, right, left)
    mine, theirs, mine_early, mine_late = lax.optimization_barrier((mine, theirs, mine[:EARLY], mine[EARLY:]))

    def rows_of(block):
        return [
            lax.ppermute(
                block,
                both,
                [
                    (device(q ^ t ^ z, c, q), device(q, c, z))
                    for q in every
                    for c in range(2)
                    for z in every
                    if z != q
                ],
            )
            for t in every
        ]

    early = rows_of(mine_early)
    same = [mine] + [
        lax.ppermute(mine, "frames", [(2 * (q ^ s) + c, 2 * q + c) for q in every for c in range(2)])
        for s in every
        if s
    ]
    late = rows_of(mine_late)
    partner = [theirs] + [lax.ppermute(same[s], "frames", swap) for s in every if s]
    info = jnp.stack([core, plane, (place // 2 == plane).astype(jnp.int32)]).astype(jnp.int32)
    product = covariance_part(info, 0, EARLY, same, partner, early, count_all, None)
    product = covariance_part(info, EARLY, 3 - EARLY, same, partner, late, count_all, product)
    return jnp.transpose(product, (0, 2, 1, 3))


def permutes_fit(planes, places):
    return places == 2 * planes and planes <= 4 and planes & (planes - 1) == 0


def general(deviation, row_count, count_all):
    panel = lax.all_gather(deviation, "frames", axis=1, tiled=True)
    ratio = lax.axis_size("frames") // lax.axis_size("atoms")
    place = lax.axis_index("frames")
    selected = lax.dynamic_slice_in_dim(panel, place % ratio * row_count, row_count, 2)
    mine = lax.axis_index("atoms") == place // ratio
    rows = lax.psum(jnp.where(mine, selected, jnp.zeros_like(selected)), "atoms")
    product = jnp.einsum("cfa,dfb->cadb", rows, panel, preferred_element_type=jnp.float32)
    return product / count_all


def whole(frames, reference_structure):
    coords = jnp.transpose(frames, (1, 0, 2))
    planes, places = lax.axis_size("atoms"), lax.axis_size("frames")
    column_atoms = frames.shape[2]
    atoms = column_atoms * planes
    count_all = frames.shape[0] * places
    row_count = atoms // places
    deviation, mean = superpose(coords, reference_structure, atoms, count_all)
    if permutes_fit(planes, places) and row_count % TILE == 0:
        covariance = direct(deviation, planes, row_count, count_all)
    else:
        covariance = general(deviation, row_count, count_all)
    return covariance, mean


def solution(mesh):
    return jax.shard_map(
        whole,
        mesh=mesh,
        in_specs=(P("frames", None, "atoms"), P(None, "atoms")),
        out_specs=(P(None, "frames", None, "atoms"), P(None, "atoms")),
        check_vma=False,
    )
```

```python
import functools

import jax
import jax.numpy as jnp
from jax import lax
from jax.experimental import pallas as pl
from jax.experimental.pallas import tpu as pltpu
from jax.sharding import PartitionSpec as P


ITERS = 2
POLAR = 8
TILE = 256
SLOTS = 4
EARLY = 1


def polar_factor(cross):
    factor = jnp.sqrt(3.0 / jnp.sum(cross * cross, axis=(0, 1)))
    matrix = cross * factor[None, None, :]
    for _ in range(POLAR):
        entries = [[matrix[i, j] for j in range(3)] for i in range(3)]
        cofactor = [
            [
                entries[(i + 1) % 3][(j + 1) % 3] * entries[(i + 2) % 3][(j + 2) % 3]
                - entries[(i + 1) % 3][(j + 2) % 3] * entries[(i + 2) % 3][(j + 1) % 3]
                for j in range(3)
            ]
            for i in range(3)
        ]
        determinant = (
            entries[0][0] * cofactor[0][0]
            + entries[0][1] * cofactor[0][1]
            + entries[0][2] * cofactor[0][2]
        )
        inverse = jnp.stack([jnp.stack(cofactor[i]) for i in range(3)]) / determinant[None, None, :]
        matrix = 0.5 * (matrix + inverse)
    return matrix


def sum_over(value, axis, steps):
    size = lax.axis_size(axis)
    if size & (size - 1) or size > 16:
        return lax.psum(value, axis)
    for masks in steps:
        value = value + sum(lax.ppermute(value, axis, [(i, i ^ m) for i in range(size)]) for m in masks)
    return value


def powers(size):
    return [[1], range(2, size, 2)] if size > 2 else [range(1, size)]


def superpose(coords, reference_structure, atoms, count_all):
    highest = lax.Precision.HIGHEST
    count = coords.shape[1]
    mean_now = reference_structure
    for iteration in range(ITERS):
        weights = mean_now
        if iteration == 0:
            weights = jnp.concatenate([mean_now, jnp.ones_like(mean_now[:1])])
        sums = jnp.einsum("cfa,da->dcf", coords, weights, precision=highest).reshape(-1, count)
        parts = [sums, jnp.broadcast_to(jnp.sum(mean_now, axis=1)[:, None], (3, count))]
        totals = sum_over(jnp.concatenate(parts), "atoms", [range(1, lax.axis_size("atoms"))])
        if iteration == 0:
            centroid = totals[9:12] / atoms
            shifted = coords - centroid[:, :, None]
        cross = totals[:9].reshape(3, 3, count).transpose(1, 0, 2) - centroid[:, None, :] * totals[-3:][None]
        rotation = polar_factor(cross)
        if iteration == ITERS - 1:
            aligned = jnp.stack(
                [sum(rotation[c, d][:, None] * shifted[c] for c in range(3)) for d in range(3)]
            )
        else:
            aligned = jnp.einsum("cdf,cfa->dfa", rotation, shifted, precision=highest)
        mean_now = sum_over(jnp.sum(aligned, axis=1), "frames", powers(lax.axis_size("frames"))) / count_all
    return (aligned - mean_now[:, None]).astype(jnp.bfloat16), mean_now


def product_kernel(count, scale, components, first, info, *refs):
    same, partner, row_blocks = refs[:count], refs[count : 2 * count], refs[2 * count : 3 * count]
    out, turned, ready, sent = refs[-4:]
    component, tile = pl.program_id(0), pl.program_id(1)
    step = 6 * component + tile
    slot = lax.rem(step, SLOTS)
    core, plane, is_hub = info[0], info[1], info[2]
    depth, row_count = same[0].shape[1], same[0].shape[2]

    def copy(c, d, half, k, m, n):
        start = pl.multiple_of(half * row_count, row_count)
        return pltpu.make_async_copy(
            ready.at[k, m : m + n],
            out.at[c + first, d, m : m + n, pl.ds(start, row_count)],
            sent.at[k],
        )

    @pl.when((tile == 0) & (is_hub == 1))
    def _():
        for s in range(count):
            turned[:, s * depth : (s + 1) * depth] = same[s][component + first].T

    @pl.when((tile == 0) & (is_hub == 0))
    def _():
        for t in range(count):
            start = pl.multiple_of((plane ^ t ^ (core * (count - 1))) * depth, depth)
            turned[:, pl.ds(start, depth)] = row_blocks[t][component].T

    @pl.when(step >= SLOTS)
    def _():
        copy(0, 0, 0, slot, 0, row_count).wait()

    def multiply(blocks):
        right = jnp.concatenate([block[lax.rem(tile, 3)] for block in blocks], axis=0)
        for m in range(0, row_count, TILE):
            value = jnp.dot(turned[m : m + TILE, :], right, preferred_element_type=jnp.float32)
            ready[slot, m : m + TILE, :] = value * (1.0 / scale) if scale & (scale - 1) == 0 else value / scale
            copy(component, lax.rem(tile, 3), core ^ (tile // 3), slot, m, TILE).start()

    @pl.when(tile < 3)
    def _():
        multiply(same)

    @pl.when(tile >= 3)
    def _():
        multiply(partner)

    @pl.when(step == 6 * components - 1)
    def _():
        for k in range(SLOTS):
            copy(0, 0, 0, k, 0, row_count).wait()


def covariance_part(info, first, components, same, partner, rows, count_all, so_far):
    count = len(same)
    depth, row_count = same[0].shape[1], same[0].shape[2]
    operands = [info, *same, *partner, *rows]
    specs = [pl.BlockSpec(memory_space=pltpu.SMEM)]
    specs += [pl.BlockSpec(memory_space=pltpu.VMEM)] * (3 * count)
    aliases = {}
    if so_far is not None:
        aliases = {len(operands): 0}
        operands.append(so_far)
        specs.append(pl.BlockSpec(memory_space=pl.ANY))
    return pl.pallas_call(
        functools.partial(product_kernel, count, count_all, components, first),
        out_shape=jax.ShapeDtypeStruct((3, 3, row_count, 2 * row_count), jnp.float32),
        grid=(components, 6),
        in_specs=specs,
        out_specs=pl.BlockSpec(memory_space=pl.ANY),
        scratch_shapes=[
            pltpu.VMEM((row_count, count * depth), jnp.bfloat16),
            pltpu.VMEM((SLOTS, row_count, row_count), jnp.float32),
            pltpu.SemaphoreType.DMA((SLOTS,)),
        ],
        input_output_aliases=aliases,
        compiler_params=pltpu.CompilerParams(
            dimension_semantics=("arbitrary", "arbitrary"), vmem_limit_bytes=24 * 2**20
        ),
        cost_estimate=pl.CostEstimate(
            flops=2 * count * depth * components * 6 * row_count * row_count,
            bytes_accessed=24 * components * row_count * row_count,
            transcendentals=0,
        ),
    )(*operands)


def direct(deviation, planes, row_count, count_all):
    def device(q, c, z):
        return (2 * q + c) * planes + z

    both = ("frames", "atoms")
    every = range(planes)
    swap = [(i, i ^ 1) for i in range(2 * planes)]
    place, plane = lax.axis_index("frames"), lax.axis_index("atoms")
    core = place % 2
    other = lax.ppermute(deviation, "frames", swap)
    lower = core == 0
    chip = jnp.concatenate([jnp.where(lower, deviation, other), jnp.where(lower, other, deviation)], axis=1)
    left, right = chip[:, :, :row_count], chip[:, :, row_count:]
    mine, theirs = jnp.where(lower, left, right), jnp.where(lower, right, left)
    mine, theirs = lax.optimization_barrier((mine, theirs))
    mine_early, mine_late = mine[:EARLY], mine[EARLY:]

    def rows_of(block):
        return [
            lax.ppermute(
                block,
                both,
                [
                    (device(q ^ t ^ z ^ (planes - 1) * c, c, q), device(q, c, z))
                    for q in every
                    for c in range(2)
                    for z in every
                    if z != q
                ],
            )
            for t in every
        ]

    early = rows_of(mine_early)
    same = [mine] + [
        lax.ppermute(mine, "frames", [(2 * (q ^ s) + c, 2 * q + c) for q in every for c in range(2)])
        for s in every
        if s
    ]
    late = rows_of(mine_late)
    partner = [theirs] + [lax.ppermute(same[s], "frames", swap) for s in every if s]
    info = jnp.stack([core, plane, (place // 2 == plane).astype(jnp.int32)]).astype(jnp.int32)
    product = covariance_part(info, 0, EARLY, same, partner, early, count_all, None)
    product = covariance_part(info, EARLY, 3 - EARLY, same, partner, late, count_all, product)
    return jnp.transpose(product, (0, 2, 1, 3))


def permutes_fit(planes, places):
    return places == 2 * planes and planes <= 4 and planes & (planes - 1) == 0


def general(deviation, row_count, count_all):
    panel = lax.all_gather(deviation, "frames", axis=1, tiled=True)
    ratio = lax.axis_size("frames") // lax.axis_size("atoms")
    place = lax.axis_index("frames")
    selected = lax.dynamic_slice_in_dim(panel, place % ratio * row_count, row_count, 2)
    mine = lax.axis_index("atoms") == place // ratio
    rows = lax.psum(jnp.where(mine, selected, jnp.zeros_like(selected)), "atoms")
    product = jnp.einsum("cfa,dfb->cadb", rows, panel, preferred_element_type=jnp.float32)
    return product / count_all


def whole(frames, reference_structure):
    coords = jnp.transpose(frames, (1, 0, 2))
    planes, places = lax.axis_size("atoms"), lax.axis_size("frames")
    column_atoms = frames.shape[2]
    atoms = column_atoms * planes
    count_all = frames.shape[0] * places
    row_count = atoms // places
    deviation, mean = superpose(coords, reference_structure, atoms, count_all)
    if permutes_fit(planes, places) and row_count % TILE == 0:
        covariance = direct(deviation, planes, row_count, count_all)
    else:
        covariance = general(deviation, row_count, count_all)
    return covariance, mean


def solution(mesh):
    return jax.shard_map(
        whole,
        mesh=mesh,
        in_specs=(P("frames", None, "atoms"), P(None, "atoms")),
        out_specs=(P(None, "frames", None, "atoms"), P(None, "atoms")),
        check_vma=False,
    )
```
